32 devices in a mesh: dp: 4 (over z), bal: 4 (over x, core), tensor: 2 (over y).
Axes of the slice: x: 2, y: 2, z: 4, core: 2. Of those that a mesh axis runs over, the one named last changes fastest.
Arguments:
- tiles: bfloat16 [4, 4, 16, 1280, 128], P('dp', 'bal', None, 'tensor'), may hold values from -6 to 6
- tile_counts: int32 [4, 4], P('dp'), may hold values from 1 to 16, 32 in all within a row
- doc_order: int32 [4, 4], P('dp'), may hold values from 0 to 3, each once within a row
- qkv_weight: bfloat16 [3, 1280, 1280], P(None, 'dp', 'tensor'), may hold values from -6 to 6
- out_weight: bfloat16 [1280, 1280], P('dp', 'tensor'), may hold values from -0.625 to 0.625
Outputs:
- encoded: bfloat16 [4, 32, 1280, 128], P('dp', 'bal', 'tensor')
The draws below stay inside these ranges and needn't reach their ends.
Inputs may be any that keep to these rules, and one draw needn't show every extreme that they name: `tile_counts`: each row sums to 32, and in every row some document has exactly 16 tiles. `doc_order`: each row names every document once.
All inputs are finite; a program needn't handle non-finite values.
Results may differ from the reference program's by a relative error of at most 0.012.
Values may be sent and summed in bfloat16 or wider, within the bound.
A program may use at most 64 MiB of HBM per device.

```python
import math
import jax
import jax.numpy as jnp
import numpy as np
from jax import lax

D = 1280
HEADS = 16
HDIM = 80
PATCH = 128
TILE_MAX = 16
CAP = 8
DOCS = 4
POSITIONS = 32
HEAD_GROUPS = 2
N_DP = 4


def draw_qkv_weight(key, part):
    standard = jnp.clip(jax.random.normal(key, (3, D, D), jnp.float32), -6.0, 6.0) * D ** (-0.5)
    return standard.astype(jnp.bfloat16)


def shard_levels(key, extent, pieces, smallest, high):
    def one(dim, shards_of):
        heights = jax.random.uniform(jax.random.fold_in(jax.random.fold_in(key, 6), dim), (shards_of,), jnp.float32, smallest / len(pieces), high / len(pieces))
        return jnp.repeat(jnp.exp(heights), extent[dim] // shards_of).reshape((-1,) + (1,) * (len(extent) - dim - 1))

    factor_of = one(*pieces[0])
    for cut in pieces[1:]:
        factor_of = factor_of * one(*cut)
    return factor_of


def length_profile(number_of, total, most, skew):
    portions = [(1 << 20) // math.isqrt(grade ** skew) + 1 for grade in range(2, number_of + 1)]
    surplus, given = total - most - (number_of - 1), [1] * (number_of - 1)
    while surplus > 0:
        candidates = [i for i in range(number_of - 1) if given[i] < most]
        mass, budget = sum([portions[i] for i in candidates]), surplus
        for i in candidates:
            more = min(most - given[i], max(1, budget * portions[i] // mass), surplus)
            given[i] = given[i] + more
            surplus = surplus - more
    return np.array([most] + given)


def ragged(own_key, amount, total, reach, skew):
    if amount == 2:
        one = jax.random.randint(own_key, (), max(1, total - reach), min(reach, total - 1) + 1)
        return jnp.stack([one, total - one])
    sizes = jnp.asarray(length_profile(amount, total, reach, skew), jnp.int32)
    couples = (amount - 1) // 2
    giver, sink = sizes[1:1 + 2 * couples:2], sizes[2:2 + 2 * couples:2]
    margin = jnp.minimum(giver - 1, reach - sink)
    shifted = jax.random.randint(jax.random.fold_in(own_key, 1), (couples,), 0, 1 << 20) % (margin + 1)
    sizes = sizes.at[1:1 + 2 * couples:2].set(giver - shifted).at[2:2 + 2 * couples:2].set(sink + shifted)
    return sizes[jax.random.permutation(jax.random.fold_in(own_key, 2), amount)]


def normal_values(rng, extent, deviation, most, split=(), kind=jnp.bfloat16):
    array = deviation * jax.random.normal(rng, extent, jnp.float32)
    if split:
        array = array * shard_levels(rng, extent, split, -0.22, 0.18)
    return jnp.clip(array, -most, most).astype(kind)


def setup_inputs(seed: int = 0) -> dict:
    key_list = jax.random.split(jax.random.key(seed), 6)
    tiles = normal_values(key_list[0], (N_DP, DOCS, TILE_MAX, D, PATCH), 1.0, 6.0, ((0, 4), (1, 4), (3, 2)))
    tile_counts = jax.vmap(lambda own: ragged(own, DOCS, POSITIONS, TILE_MAX, 2))(jax.random.split(key_list[1], N_DP)).reshape((N_DP, DOCS)).astype(jnp.int32)
    doc_order = jax.vmap(lambda own: jax.random.permutation(own, DOCS))(jax.random.split(key_list[2], N_DP)).reshape((N_DP, DOCS)).astype(jnp.int32)
    qkv_weight = draw_qkv_weight(jax.random.fold_in(key_list[5], 71), 0)
    out_weight = normal_values(key_list[4], (D, D), HDIM ** -0.5, 0.625, ((0, 4), (1, 2)))
    return {"tiles": tiles, "tile_counts": tile_counts, "doc_order": doc_order, "qkv_weight": qkv_weight, "out_weight": out_weight}


EPSILON = 1e-06

def normalize(tile_rows):
    values = tile_rows.astype(jnp.float32)
    center = values - lax.optimization_barrier(jnp.mean(values, axis=-1, keepdims=True))
    spread = lax.optimization_barrier(jnp.mean(center * center, axis=-1, keepdims=True))
    return (center * lax.rsqrt(spread + EPSILON)).astype(jnp.bfloat16)

def encode(tile_block, qkv_weight, out_weight):
    tile_total = tile_block.shape[0]
    row_count = tile_total * PATCH
    normed = normalize(tile_block).reshape(row_count, D)
    flat_weight = jnp.transpose(qkv_weight, (1, 0, 2)).reshape(D, 3 * D)
    projected = jnp.dot(normed, flat_weight, preferred_element_type=jnp.float32).astype(jnp.bfloat16)
    projected = projected.reshape(tile_total, PATCH, 3, HEADS, HDIM)
    query = projected[:, :, 0].astype(jnp.float32)
    key_rows = projected[:, :, 1].astype(jnp.float32)
    value_rows = projected[:, :, 2].astype(jnp.float32)
    scores = jnp.einsum('rqhe,rkhe->rhqk', query, key_rows) * HDIM ** (-0.5)
    probs = jax.nn.softmax(scores, axis=-1).astype(jnp.bfloat16)
    context = jnp.einsum('rhqk,rkhe->rqhe', probs.astype(jnp.float32), value_rows).astype(jnp.bfloat16)
    context = context.reshape(row_count, D)
    group_width = D // HEAD_GROUPS
    running = tile_block.astype(jnp.float32).reshape(row_count, D)
    for group in range(HEAD_GROUPS):
        low = group * group_width
        partial_value = jnp.dot(context[:, low:low + group_width], out_weight[:, low:low + group_width].T, preferred_element_type=jnp.float32)
        rounded = lax.optimization_barrier(partial_value.astype(jnp.bfloat16))
        running = running + rounded.astype(jnp.float32)
    return running.astype(jnp.bfloat16).reshape(tile_total, PATCH, D)

def reference(tiles, tile_counts, doc_order, qkv_weight, out_weight):
    doc_ids = jnp.arange(DOCS, dtype=jnp.int32)

    def group_index(counts, ordering):
        position = lax.optimization_barrier(jnp.sum(jnp.where(ordering[None, :] == doc_ids[:, None], doc_ids[None, :], 0), axis=1))
        starts = lax.optimization_barrier(jnp.sum(jnp.where(position[None, :] < position[:, None], counts[None, :], 0), axis=1))
        packed = jnp.arange(POSITIONS, dtype=jnp.int32)
        inside = (starts[None, :] <= packed[:, None]) & (packed[:, None] < (starts + counts)[None, :])
        source = lax.optimization_barrier(jnp.sum(jnp.where(inside, doc_ids[None, :], 0), axis=1))
        offset = packed - lax.optimization_barrier(jnp.sum(jnp.where(inside, starts[None, :], 0), axis=1))
        return (source * TILE_MAX + offset).astype(jnp.int32)
    flat_index = jax.vmap(group_index)(tile_counts, doc_order)
    group_base = (jnp.arange(N_DP, dtype=jnp.int32) * (DOCS * TILE_MAX)).astype(jnp.int32)
    flat_index = (flat_index + group_base[:, None]).astype(jnp.int32)
    flat_tiles = jnp.swapaxes(tiles, 3, 4).reshape(N_DP * DOCS * TILE_MAX, PATCH, D)
    packed_tiles = jnp.take(flat_tiles, flat_index.reshape(-1), axis=0)
    blocks = packed_tiles.reshape(N_DP * POSITIONS // CAP, CAP, PATCH, D)
    encoded = lax.map(lambda tile_block: encode(tile_block, qkv_weight, out_weight), blocks)
    return jnp.swapaxes(encoded.reshape(N_DP, POSITIONS, PATCH, D), 2, 3)
```

```python
import functools

import jax
import jax.numpy as jnp
from jax import lax
from jax.experimental import pallas as pl
from jax.experimental.pallas import tpu as pltpu
from jax.sharding import PartitionSpec as P

HDIM = 80
CAP = 8
CHUNK = 2
EPSILON = 1e-06
MESH = pl.DeviceIdType.MESH


def flip(index, bit):
    return index + bit - 2 * bit * ((index // bit) % 2)


def bits_of(size):
    bits = []
    while 1 << len(bits) < size:
        bits.append(1 << len(bits))
    return bits


def remote(src, dst, send, recv, **device):
    return pltpu.make_async_remote_copy(
        src_ref=src, dst_ref=dst, send_sem=send, recv_sem=recv, device_id=device, device_id_type=MESH
    )


def gather_kernel(sizes, *refs):
    nd, nb, nt = sizes
    bits = bits_of(nb)
    ns = len(bits)
    tab, tiles, wq_in, wo_in, gath, wq, wo = refs[:7]
    sends, recvs = refs[7 : 7 + ns], refs[7 + ns : 7 + 2 * ns]
    t_send, t_recv, y_send, y_recv, w_send, w_recv, d_send, d_recv = refs[7 + 2 * ns :]
    z, b, t = lax.axis_index("dp"), lax.axis_index("bal"), lax.axis_index("tensor")
    slices = tiles.shape[1]
    chunks = CAP // CHUNK

    barrier = pltpu.get_barrier_semaphore()
    for m in bits:
        pl.semaphore_signal(barrier, inc=1, device_id={"bal": flip(b, m)}, device_id_type=MESH)
    for j in range(1, nt):
        pl.semaphore_signal(barrier, inc=1, device_id={"tensor": (t + j) % nt}, device_id_type=MESH)

    def greet(j, carry):
        pl.semaphore_signal(barrier, inc=1, device_id={"dp": (z + j) % nd}, device_id_type=MESH)
        return carry

    lax.fori_loop(1, nd, greet, 0)
    pl.semaphore_wait(barrier, ns + nt - 1 + nd - 1)

    pairs = ((wq_in, wq), (wo_in, wo))

    def spread(j, a):
        src, dst = pairs[a]
        return remote(
            src.at[b], dst.at[z, b], w_send.at[a, j], w_recv.at[a, j], dp=(z + j) % nd
        )

    for a in range(2):

        def start_spread(j, carry, a=a):
            spread(j, a).start()
            return carry

        lax.fori_loop(1, nd, start_spread, 0)

    def tile_copy(s, slot, c):
        part = pl.ds(c * CHUNK, CHUNK)
        return remote(
            sends[s].at[slot, part],
            recvs[s].at[slot, part],
            t_send.at[s, slot, c],
            t_recv.at[s, slot, c],
            bal=flip(b, bits[s]),
        )

    def slot_of(s, r):
        return r >> (s + 1)

    def wait_for(s, r, c):
        for q in range(s):
            tile_copy(q, slot_of(q, r), c).wait_recv()

    def current(s, r, i):
        value = tiles[tab[0, r * CAP + i]]
        for q in range(s):
            value = lax.select(
                tab[1 + q, r * CAP + i] != 0, recvs[q][slot_of(q, r), i], value
            )
        return value

    for s, m in enumerate(bits):
        wanted = [r for r in range(nb) if r & (m - 1) == 0 and r & m]
        for r in reversed(wanted):
            slot = slot_of(s, r - m)
            for c in range(chunks):
                wait_for(s, r, c)

                def fill(i, carry, s=s, r=r, slot=slot):
                    sends[s][slot, i] = current(s, r, i)
                    return carry

                lax.fori_loop(c * CHUNK, (c + 1) * CHUNK, fill, 0)
                tile_copy(s, slot, c).start()

    mine = pl.ds(pl.multiple_of(t * slices, 16), slices)

    def y_copy(c, j):
        part = gath.at[pl.ds(c * CHUNK, CHUNK), mine, :]
        return remote(part, part, y_send.at[c, j], y_recv.at[c, j], tensor=(t + j) % nt)

    for c in range(chunks):
        wait_for(ns, 0, c)

        def settle(i, carry):
            gath[i, mine, :] = current(ns, 0, i)
            return carry

        lax.fori_loop(c * CHUNK, (c + 1) * CHUNK, settle, 0)
        for j in range(1, nt):
            y_copy(c, j).start()

    for a in range(2):
        src, dst = pairs[a]
        dst[z] = src[...]

    def doubled(j, a, s, e):
        src = (z + nd - j) % nd
        held = b
        for q in range(s):
            if (e >> q) & 1:
                held = flip(held, bits[ns - 1 - q])
        dst = pairs[a][1].at[src, held]
        at = (1 << s) - 1 + e
        return remote(
            dst, dst, d_send.at[a, j, at], d_recv.at[a, j, at], bal=flip(b, bits[ns - 1 - s])
        )

    for a in range(2):

        def first(j, carry, a=a):
            spread(j, a).wait_recv()
            doubled(j, a, 0, 0).start()
            return carry

        lax.fori_loop(1, nd, first, 0)
    for s in range(1, ns + 1):
        for a in range(2):

            def further(j, carry, a=a, s=s):
                for e in range(1 << (s - 1)):
                    doubled(j, a, s - 1, e).wait_recv()
                if s < ns:
                    for e in range(1 << s):
                        doubled(j, a, s, e).start()
                return carry

            lax.fori_loop(1, nd, further, 0)

    for c in range(chunks):
        for j in range(1, nt):
            y_copy(c, j).wait_recv()
            y_copy(c, j).wait_send()
    for s, m in enumerate(bits):
        for slot in range(nb >> (s + 1)):
            for c in range(chunks):
                tile_copy(s, slot, c).wait_send()
    for a in range(2):

        def drain(j, carry, a=a):
            spread(j, a).wait_send()
            for s in range(ns):
                for e in range(1 << s):
                    doubled(j, a, s, e).wait_send()
            return carry

        lax.fori_loop(1, nd, drain, 0)


def gather_all(table, tiles, qkv_weight, out_weight):
    nd, nb, nt = (lax.axis_size(name) for name in ("dp", "bal", "tensor"))
    ns = len(bits_of(nb))
    slots, slices, patches = tiles.shape
    columns = qkv_weight.shape[-1]
    wq = qkv_weight.reshape(nb, -1, columns)
    wo = out_weight.reshape(nb, -1, columns)
    chunks = CAP // CHUNK
    dtype = tiles.dtype
    vmem = pl.BlockSpec(memory_space=pltpu.VMEM)
    dma = pltpu.SemaphoreType.DMA
    buffers = [pltpu.VMEM((nb >> (s + 1), CAP, slices, patches), dtype) for s in range(ns)]
    gathered, full_qkv, full_out = pl.pallas_call(
        functools.partial(gather_kernel, (nd, nb, nt)),
        out_shape=(
            jax.ShapeDtypeStruct((CAP, nt * slices, patches), dtype),
            jax.ShapeDtypeStruct((nd,) + wq.shape, dtype),
            jax.ShapeDtypeStruct((nd,) + wo.shape, dtype),
        ),
        in_specs=[pl.BlockSpec(memory_space=pltpu.SMEM), vmem, vmem, vmem],
        out_specs=(vmem, vmem, vmem),
        scratch_shapes=buffers
        + buffers
        + [dma((ns, max(nb // 2, 1), chunks))] * 2
        + [dma((chunks, nt))] * 2
        + [dma((2, nd))] * 2
        + [dma((2, nd, nb))] * 2,
        compiler_params=pltpu.CompilerParams(
            collective_id=0, has_side_effects=True, vmem_limit_bytes=50 * 1024 * 1024
        ),
        name="gather_all",
    )(table, tiles, wq, wo)
    return (
        gathered,
        full_qkv.reshape((nd,) + qkv_weight.shape),
        full_out.reshape((-1, columns)),
    )


def route(counts, ordering, slot_count):
    nb, b = lax.axis_size("bal"), lax.axis_index("bal")
    doc_ids = jnp.arange(counts.shape[0], dtype=jnp.int32)
    position = jnp.sum(
        jnp.where(ordering[None, :] == doc_ids[:, None], doc_ids[None, :], 0), axis=1
    )
    starts = jnp.sum(jnp.where(position[None, :] < position[:, None], counts[None, :], 0), axis=1)
    own_start = jnp.sum(jnp.where(doc_ids == b, starts, 0))
    relative = jnp.arange(nb * CAP, dtype=jnp.int32)
    packed = ((relative // CAP) ^ b) * CAP + relative % CAP
    inside = (starts[:, None] <= packed[None, :]) & (packed[None, :] < (starts + counts)[:, None])
    owner = jnp.sum(jnp.where(inside, doc_ids[:, None], 0), axis=0)
    rows = [jnp.clip(packed - own_start, 0, slot_count - 1)]
    for m in bits_of(nb):
        rows.append(((owner ^ b) // m) % 2)
    return jnp.stack(rows)


def normalize(tile_rows):
    values = tile_rows.astype(jnp.float32)
    center = values - jnp.mean(values, axis=1, keepdims=True)
    spread = jnp.mean(center * center, axis=1, keepdims=True)
    return (center * lax.rsqrt(spread + EPSILON)).astype(jnp.bfloat16)


def local(tiles, tile_counts, doc_order, qkv_weight, out_weight):
    own_tiles = tiles[0, 0]
    slot_count, slices, patches = own_tiles.shape
    table = route(tile_counts[0], doc_order[0], slot_count)
    gathered, full_qkv, full_out = gather_all(table, own_tiles, qkv_weight, out_weight)
    t = lax.axis_index("tensor")
    chosen = lax.dynamic_slice_in_dim(gathered, t * slices, slices, axis=1)
    normed = normalize(gathered)
    full_qkv = full_qkv.transpose(1, 0, 2, 3).reshape(3, -1, slices)
    projected = jnp.einsum("cdp,kdf->kcfp", normed, full_qkv, preferred_element_type=jnp.float32)
    head_count = slices // HDIM
    projected = projected.astype(jnp.bfloat16).reshape(3, CAP, head_count, HDIM, patches)
    scores = jnp.einsum(
        "rhet,rhes->rhts", projected[0], projected[1], preferred_element_type=jnp.float32
    ) * HDIM ** (-0.5)
    probs = jax.nn.softmax(scores, axis=-1).astype(jnp.bfloat16)
    context = jnp.einsum("rhts,rhes->rhet", probs, projected[2], preferred_element_type=jnp.float32)
    context = context.astype(jnp.bfloat16).reshape(CAP, slices, patches)
    partial_value = jnp.einsum("cep,fe->cfp", context, full_out, preferred_element_type=jnp.float32)
    summed = lax.psum_scatter(
        partial_value.astype(jnp.bfloat16), "tensor", scatter_dimension=1, tiled=True
    ).astype(jnp.float32)
    return (chosen.astype(jnp.float32) + summed).astype(jnp.bfloat16)[None]


def solution(mesh):
    placed = (
        P("dp", "bal", None, "tensor", None),
        P("dp", None),
        P("dp", None),
        P(None, "dp", "tensor"),
        P("dp", "tensor"),
    )
    return jax.shard_map(
        local, mesh=mesh, in_specs=placed, out_specs=P("dp", "bal", "tensor", None), check_vma=False
    )
```

```python
import functools

import jax
import jax.numpy as jnp
from jax import lax
from jax.experimental import pallas as pl
from jax.experimental.pallas import tpu as pltpu
from jax.sharding import PartitionSpec as P

HDIM = 80
CAP = 8
CHUNK = 2
EPSILON = 1e-06
MESH = pl.DeviceIdType.MESH


def flip(index, bit):
    return index + bit - 2 * bit * ((index // bit) % 2)


def bits_of(size):
    bits = []
    while 1 << len(bits) < size:
        bits.append(1 << len(bits))
    return bits


def remote(src, dst, send, recv, **device):
    return pltpu.make_async_remote_copy(
        src_ref=src, dst_ref=dst, send_sem=send, recv_sem=recv, device_id=device, device_id_type=MESH
    )


def encode_kernel(sizes, *refs):
    nd, nb, nt = sizes
    bits = bits_of(nb)
    ns = len(bits)
    tab, tiles, wq_in, wo_in, out = refs[:5]
    sends, recvs = refs[5 : 5 + ns], refs[5 + ns : 5 + 2 * ns]
    gath, wq, wo, wide_q, wide_o, normed, qkv, context, own, p_out, p_in = refs[
        5 + 2 * ns : 16 + 2 * ns
    ]
    t_send, t_recv, y_send, y_recv, w_send, w_recv, d_send, d_recv, p_send, p_recv = refs[
        16 + 2 * ns :
    ]
    z, b, t = lax.axis_index("dp"), lax.axis_index("bal"), lax.axis_index("tensor")
    _, slices, patches = tiles.shape
    chunks = CAP // CHUNK

    barrier = pltpu.get_barrier_semaphore()
    for m in bits:
        pl.semaphore_signal(barrier, inc=1, device_id={"bal": flip(b, m)}, device_id_type=MESH)
    for j in range(1, nt):
        pl.semaphore_signal(barrier, inc=1, device_id={"tensor": (t + j) % nt}, device_id_type=MESH)

    def greet(j, carry):
        pl.semaphore_signal(barrier, inc=1, device_id={"dp": (z + j) % nd}, device_id_type=MESH)
        return carry

    lax.fori_loop(1, nd, greet, 0)
    pl.semaphore_wait(barrier, ns + nt - 1 + nd - 1)

    pairs = ((wq_in, wq), (wo_in, wo))

    def spread(j, a):
        src, dst = pairs[a]
        return remote(
            src.at[b], dst.at[z, b], w_send.at[a, j], w_recv.at[a, j], dp=(z + j) % nd
        )

    for a in range(2):

        def start_spread(j, carry, a=a):
            spread(j, a).start()
            return carry

        lax.fori_loop(1, nd, start_spread, 0)

    def tile_copy(s, slot, c):
        part = pl.ds(c * CHUNK, CHUNK)
        return remote(
            sends[s].at[slot, part],
            recvs[s].at[slot, part],
            t_send.at[s, slot, c],
            t_recv.at[s, slot, c],
            bal=flip(b, bits[s]),
        )

    def slot_of(s, r):
        return r >> (s + 1)

    def wait_for(s, r, c):
        for q in range(s):
            tile_copy(q, slot_of(q, r), c).wait_recv()

    def current(s, r, i):
        value = tiles[tab[0, r * CAP + i]]
        for q in range(s):
            value = lax.select(
                tab[1 + q, r * CAP + i] != 0, recvs[q][slot_of(q, r), i], value
            )
        return value

    for s, m in enumerate(bits):
        wanted = [r for r in range(nb) if r & (m - 1) == 0 and r & m]
        for r in reversed(wanted):
            slot = slot_of(s, r - m)
            for c in range(chunks):
                wait_for(s, r, c)

                def fill(i, carry, s=s, r=r, slot=slot):
                    sends[s][slot, i] = current(s, r, i)
                    return carry

                lax.fori_loop(c * CHUNK, (c + 1) * CHUNK, fill, 0)
                tile_copy(s, slot, c).start()

    mine = pl.ds(pl.multiple_of(t * slices, 16), slices)

    def y_copy(c, j):
        part = gath.at[pl.ds(c * CHUNK, CHUNK), mine, :]
        return remote(part, part, y_send.at[c, j], y_recv.at[c, j], tensor=(t + j) % nt)

    for c in range(chunks):
        wait_for(ns, 0, c)

        def settle(i, carry):
            gath[i, mine, :] = current(ns, 0, i)
            return carry

        lax.fori_loop(c * CHUNK, (c + 1) * CHUNK, settle, 0)
        for j in range(1, nt):
            y_copy(c, j).start()

    for a in range(2):
        src, dst = pairs[a]
        dst[z] = src[...]

    def doubled(j, a, s, e):
        src = (z + nd - j) % nd
        held = b
        for q in range(s):
            if (e >> q) & 1:
                held = flip(held, bits[ns - 1 - q])
        dst = pairs[a][1].at[src, held]
        at = (1 << s) - 1 + e
        return remote(
            dst, dst, d_send.at[a, j, at], d_recv.at[a, j, at], bal=flip(b, bits[ns - 1 - s])
        )

    for a in range(2):

        def first(j, carry, a=a):
            spread(j, a).wait_recv()
            doubled(j, a, 0, 0).start()
            return carry

        lax.fori_loop(1, nd, first, 0)
    def finish(a):
        for s in range(1, ns + 1):

            def further(j, carry, s=s):
                for e in range(1 << (s - 1)):
                    doubled(j, a, s - 1, e).wait_recv()
                if s < ns:
                    for e in range(1 << s):
                        doubled(j, a, s, e).start()
                return carry

            lax.fori_loop(1, nd, further, 0)

    for c in range(chunks):
        for j in range(1, nt):
            y_copy(c, j).wait_recv()
    for i in range(CAP):
        values = gath[i].astype(jnp.float32)
        center = values - jnp.mean(values, axis=0, keepdims=True)
        spread_of = jnp.mean(center * center, axis=0, keepdims=True)
        normed[:, i * patches : (i + 1) * patches] = (
            center * lax.rsqrt(spread_of + EPSILON)
        ).astype(normed.dtype)

    finish(0)
    rows = wide_q.shape[1] // nd
    part_rows = wq.shape[2]
    for y in range(nd):
        for e in range(nb):
            at = 0
            while at < part_rows:
                k, row = divmod(e * part_rows + at, rows)
                size = min(rows - row, part_rows - at)
                wide_q[k, y * rows + row : y * rows + row + size] = wq[y, e, at : at + size]
                at += size

    def project(k, carry):
        qkv[k] = lax.dot_general(
            wide_q[k], normed[...], (((0,), (0,)), ((), ())), preferred_element_type=jnp.float32
        ).astype(qkv.dtype)
        return carry

    lax.fori_loop(0, 3, project, 0)
    finish(1)
    part_rows = wo.shape[2]
    for y in range(nd):
        for e in range(nb):
            start = (y * nb + e) * part_rows
            wide_o[start : start + part_rows] = wo[y, e]

    def p_copy(c, j):
        part = pl.ds(c * CHUNK, CHUNK)
        return remote(
            p_out.at[j - 1, part], p_in.at[j - 1, part], p_send.at[c, j], p_recv.at[c, j],
            tensor=(t + j) % nt,
        )

    heads = slices // HDIM

    def partial(target):
        block = wide_o[pl.ds(pl.multiple_of(target * slices, 16), slices), :]
        return jnp.dot(block, context[...], preferred_element_type=jnp.float32).astype(own.dtype)

    def encode(c, carry):
        for i in range(CHUNK):
            here = pl.ds(pl.multiple_of((c * CHUNK + i) * patches, patches), patches)
            for h in range(heads):
                span = slice(h * HDIM, (h + 1) * HDIM)
                scores = lax.dot_general(
                    qkv[1, span, here], qkv[0, span, here], (((0,), (0,)), ((), ())),
                    preferred_element_type=jnp.float32,
                ) * HDIM ** (-0.5)
                powers = jnp.exp(scores - jnp.max(scores, axis=0, keepdims=True))
                probs = powers * (1.0 / jnp.sum(powers, axis=0, keepdims=True))
                context[span, i * patches : (i + 1) * patches] = jnp.dot(
                    qkv[2, span, here], probs.astype(qkv.dtype), preferred_element_type=jnp.float32
                ).astype(context.dtype)
        for j in range(1, nt):
            block = partial((t + j) % nt)
            for i in range(CHUNK):
                p_out[j - 1, c * CHUNK + i] = block[:, i * patches : (i + 1) * patches]
            p_copy(c, j).start()
        block = partial(t)
        for i in range(CHUNK):
            own[c * CHUNK + i] = block[:, i * patches : (i + 1) * patches]
        return carry

    lax.fori_loop(0, chunks, encode, 0)

    def close(c, carry):
        for j in range(1, nt):
            p_copy(c, j).wait_recv()
        for i in range(CHUNK):
            at = c * CHUNK + i
            total = gath[at, mine, :].astype(jnp.float32) + own[at].astype(jnp.float32)
            for j in range(1, nt):
                total = total + p_in[j - 1, at].astype(jnp.float32)
            out[at] = total.astype(out.dtype)
        return carry

    lax.fori_loop(0, chunks, close, 0)

    for c in range(chunks):
        for j in range(1, nt):
            y_copy(c, j).wait_send()
            p_copy(c, j).wait_send()
    for s, m in enumerate(bits):
        for slot in range(nb >> (s + 1)):
            for c in range(chunks):
                tile_copy(s, slot, c).wait_send()
    for a in range(2):

        def drain(j, carry, a=a):
            spread(j, a).wait_send()
            for s in range(ns):
                for e in range(1 << s):
                    doubled(j, a, s, e).wait_send()
            return carry

        lax.fori_loop(1, nd, drain, 0)


def encode_all(table, tiles, qkv_weight, out_weight):
    nd, nb, nt = (lax.axis_size(name) for name in ("dp", "bal", "tensor"))
    ns = len(bits_of(nb))
    slots, slices, patches = tiles.shape
    kinds, rows, columns = qkv_weight.shape
    wq = qkv_weight.reshape(nb, -1, columns)
    wo = out_weight.reshape(nb, -1, columns)
    chunks = CAP // CHUNK
    dtype = tiles.dtype
    vmem = pl.BlockSpec(memory_space=pltpu.VMEM)
    dma = pltpu.SemaphoreType.DMA

    def space(*shape):
        return pltpu.VMEM(shape, dtype)

    buffers = [space(nb >> (s + 1), CAP, slices, patches) for s in range(ns)]
    return pl.pallas_call(
        functools.partial(encode_kernel, (nd, nb, nt)),
        out_shape=jax.ShapeDtypeStruct((CAP, slices, patches), dtype),
        in_specs=[pl.BlockSpec(memory_space=pltpu.SMEM), vmem, vmem, vmem],
        out_specs=vmem,
        scratch_shapes=buffers
        + buffers
        + [
            space(CAP, nt * slices, patches),
            space(nd, *wq.shape),
            space(nd, *wo.shape),
            space(kinds, nd * rows, columns),
            space(nt * slices, columns),
            space(nt * slices, CAP * patches),
            space(kinds, columns, CAP * patches),
            space(columns, CHUNK * patches),
            space(CAP, slices, patches),
            space(max(nt - 1, 1), CAP, slices, patches),
            space(max(nt - 1, 1), CAP, slices, patches),
        ]
        + [dma((ns, max(nb // 2, 1), chunks))] * 2
        + [dma((chunks, nt))] * 2
        + [dma((2, nd))] * 2
        + [dma((2, nd, nb))] * 2
        + [dma((chunks, nt))] * 2,
        compiler_params=pltpu.CompilerParams(
            collective_id=0, has_side_effects=True, vmem_limit_bytes=60 * 1024 * 1024
        ),
        name="encode_all",
    )(table, tiles, wq, wo)


def route(counts, ordering, slot_count):
    nb, b = lax.axis_size("bal"), lax.axis_index("bal")
    doc_ids = jnp.arange(counts.shape[0], dtype=jnp.int32)
    position = jnp.sum(
        jnp.where(ordering[None, :] == doc_ids[:, None], doc_ids[None, :], 0), axis=1
    )
    starts = jnp.sum(jnp.where(position[None, :] < position[:, None], counts[None, :], 0), axis=1)
    own_start = jnp.sum(jnp.where(doc_ids == b, starts, 0))
    relative = jnp.arange(nb * CAP, dtype=jnp.int32)
    packed = ((relative // CAP) ^ b) * CAP + relative % CAP
    inside = (starts[:, None] <= packed[None, :]) & (packed[None, :] < (starts + counts)[:, None])
    owner = jnp.sum(jnp.where(inside, doc_ids[:, None], 0), axis=0)
    rows = [jnp.clip(packed - own_start, 0, slot_count - 1)]
    for m in bits_of(nb):
        rows.append(((owner ^ b) // m) % 2)
    return jnp.stack(rows)


def local(tiles, tile_counts, doc_order, qkv_weight, out_weight):
    own_tiles = tiles[0, 0]
    table = route(tile_counts[0], doc_order[0], own_tiles.shape[0])
    return encode_all(table, own_tiles, qkv_weight, out_weight)[None]


def solution(mesh):
    placed = (
        P("dp", "bal", None, "tensor", None),
        P("dp", None),
        P("dp", None),
        P(None, "dp", "tensor"),
        P("dp", "tensor"),
    )
    return jax.shard_map(
        local, mesh=mesh, in_specs=placed, out_specs=P("dp", "bal", "tensor", None), check_vma=False
    )
```

```python
import functools

import jax
import jax.numpy as jnp
from jax import lax
from jax.experimental import pallas as pl
from jax.experimental.pallas import tpu as pltpu
from jax.sharding import PartitionSpec as P

HDIM = 80
CAP = 8
CHUNK = 2
EPSILON = 1e-06
MESH = pl.DeviceIdType.MESH


def flip(index, bit):
    return index + bit - 2 * bit * ((index // bit) % 2)


def bits_of(size):
    bits = []
    while 1 << len(bits) < size:
        bits.append(1 << len(bits))
    return bits


def remote(src, dst, send, recv, **device):
    return pltpu.make_async_remote_copy(
        src_ref=src, dst_ref=dst, send_sem=send, recv_sem=recv, device_id=device, device_id_type=MESH
    )


def encode_kernel(sizes, *refs):
    nd, nb, nt = sizes
    bits = bits_of(nb)
    ns = len(bits)
    counts, order, tiles, wq_in, wo_in, out = refs[:6]
    sends, recvs = refs[6 : 6 + ns], refs[6 + ns : 6 + 2 * ns]
    gath, wq, wo, wide_o, normed, qkv, context, own, p_out, p_in = refs[6 + 2 * ns : 16 + 2 * ns]
    sems = refs[16 + 2 * ns :]
    t_send, t_recv, y_send, y_recv, w_send, w_recv, d_send, d_recv, p_send, p_recv = sems[:10]
    l_send, l_recv, h_send, h_recv = sems[10:]
    z, b, t = lax.axis_index("dp"), lax.axis_index("bal"), lax.axis_index("tensor")
    _, slices, patches = tiles.shape
    chunks = CAP // CHUNK

    barrier = pltpu.get_barrier_semaphore()
    for m in bits:
        pl.semaphore_signal(barrier, inc=1, device_id={"bal": flip(b, m)}, device_id_type=MESH)
    for j in range(1, nt):
        pl.semaphore_signal(barrier, inc=1, device_id={"tensor": (t + j) % nt}, device_id_type=MESH)

    def greet(j, carry):
        pl.semaphore_signal(barrier, inc=1, device_id={"dp": (z + j) % nd}, device_id_type=MESH)
        return carry

    lax.fori_loop(1, nd, greet, 0)
    pl.semaphore_wait(barrier, ns + nt - 1 + nd - 1)

    def spread(j):
        return remote(wo_in.at[b], wo.at[z, b], w_send.at[j], w_recv.at[j], dp=(z + j) % nd)

    part_count = wq.shape[2]
    part = b % part_count

    def line(way, s):
        step = 1 - 2 * way
        src = z - step * s
        there = z + step
        valid = (src >= 0) & (src < nd) & (there >= 0) & (there < nd)
        dst = wq.at[:, jnp.clip(src, 0, nd - 1), part]
        origin = wq_in.at[:, part] if isinstance(s, int) and s == 0 else dst
        copy = remote(
            origin, dst, l_send.at[way, s], l_recv.at[way, s], dp=jnp.clip(there, 0, nd - 1)
        )
        return valid, copy

    def arrival(way, s):
        step = 1 - 2 * way
        src = z - step * (s + 1)
        valid = (src >= 0) & (src < nd)
        at = wq.at[:, jnp.clip(src, 0, nd - 1), part]
        here = remote(
            at, at, l_send.at[way, s], l_recv.at[way, s], dp=jnp.clip(z + step, 0, nd - 1)
        )
        half = remote(at, at, h_send.at[way, s], h_recv.at[way, s], bal=flip(b, 1))
        return valid, here, half

    for way in range(2):
        valid, copy = line(way, 0)
        pl.when(valid)(copy.start)

    def hop(s):
        for way in range(2):
            valid, here, half = arrival(way, s)
            further, copy = line(way, s + 1)

            @pl.when(valid)
            def _(here=here, half=half, further=further, copy=copy):
                here.wait_recv()
                pl.when(further)(copy.start)
                if part_count > 1:
                    half.start()

    def tile_copy(s, slot, c):
        part = pl.ds(c * CHUNK, CHUNK)
        return remote(
            sends[s].at[slot, part],
            recvs[s].at[slot, part],
            t_send.at[s, slot, c],
            t_recv.at[s, slot, c],
            bal=flip(b, bits[s]),
        )

    def slot_of(s, r):
        return r >> (s + 1)

    def wait_for(s, r, c):
        for q in range(s):
            tile_copy(q, slot_of(q, r), c).wait_recv()

    docs = order.shape[1]
    placed = [order[0, p] for p in range(docs)]
    edges = [jnp.int32(0)]
    for doc in placed:
        edges.append(edges[-1] + counts[0, doc])
    own_start = jnp.int32(0)
    for p in range(docs):
        own_start = own_start + jnp.where(placed[p] == b, edges[p], 0)

    def current(s, r, i):
        block = b
        for m in bits:
            if r & m:
                block = flip(block, m)
        packed = block * CAP + i
        owner = jnp.int32(0)
        for p in range(docs):
            inside = (edges[p] <= packed) & (packed < edges[p + 1])
            owner = owner + jnp.where(inside, placed[p], 0)
        value = tiles[jnp.clip(packed - own_start, 0, tiles.shape[0] - 1)]
        for q in range(s):
            apart = (owner // bits[q]) % 2 != (b // bits[q]) % 2
            value = lax.select(apart, recvs[q][slot_of(q, r), i], value)
        return value

    for s, m in enumerate(bits):
        wanted = [r for r in range(nb) if r & (m - 1) == 0 and r & m]
        for r in reversed(wanted):
            slot = slot_of(s, r - m)
            for c in range(chunks):
                wait_for(s, r, c)

                def fill(i, carry, s=s, r=r, slot=slot):
                    sends[s][slot, i] = current(s, r, i)
                    return carry

                lax.fori_loop(c * CHUNK, (c + 1) * CHUNK, fill, 0)
                tile_copy(s, slot, c).start()

    mine = pl.ds(pl.multiple_of(t * slices, 16), slices)

    def y_copy(c, j):
        part = gath.at[pl.ds(c * CHUNK, CHUNK), mine, :]
        return remote(part, part, y_send.at[c, j], y_recv.at[c, j], tensor=(t + j) % nt)

    early = min((chunks + 1) // 2, nd - 2)
    for c in range(chunks):
        wait_for(ns, 0, c)

        def settle(i, carry):
            gath[i, mine, :] = current(ns, 0, i)
            return carry

        lax.fori_loop(c * CHUNK, (c + 1) * CHUNK, settle, 0)
        for j in range(1, nt):
            y_copy(c, j).start()
        if c % 2 == 0 and c // 2 < early:
            hop(c // 2)

    def start_spread(j, carry):
        spread(j).start()
        return carry

    lax.fori_loop(1, nd, start_spread, 0)
    wq[:, z] = wq_in[...]
    wo[z] = wo_in[...]

    def doubled(j, s, e):
        src = (z + nd - j) % nd
        held = b
        for q in range(s):
            if (e >> q) & 1:
                held = flip(held, bits[ns - 1 - q])
        dst = wo.at[src, held]
        at = (1 << s) - 1 + e
        return remote(
            dst, dst, d_send.at[j, at], d_recv.at[j, at], bal=flip(b, bits[ns - 1 - s])
        )

    def finish(s):
        def further(j, carry):
            if s == 0:
                spread(j).wait_recv()
            else:
                for e in range(1 << (s - 1)):
                    doubled(j, s - 1, e).wait_recv()
            if s < ns:
                for e in range(1 << s):
                    doubled(j, s, e).start()
            return carry

        lax.fori_loop(1, nd, further, 0)

    def normalize(i):
        values = gath[i].astype(jnp.float32)
        center = values - jnp.mean(values, axis=0, keepdims=True)
        spread_of = jnp.mean(center * center, axis=0, keepdims=True)
        normed[:, i * patches : (i + 1) * patches] = (
            center * lax.rsqrt(spread_of + EPSILON)
        ).astype(normed.dtype)

    for c in range(chunks):
        for j in range(1, nt):
            y_copy(c, j).wait_recv()
        for i in range(c * CHUNK, (c + 1) * CHUNK):
            normalize(i)

    def rest(s, carry):
        hop(s)
        return carry

    lax.fori_loop(early, nd - 1, rest, 0)
    finish(0)

    def halves(s, carry):
        for way in range(2):
            valid, _, half = arrival(way, s)
            pl.when(valid)(half.wait_recv)
        return carry

    if part_count > 1:
        lax.fori_loop(0, nd - 1, halves, 0)

    def project(k, carry):
        qkv[k] = lax.dot_general(
            wq[k].reshape(normed.shape[0], slices),
            normed[...],
            (((0,), (0,)), ((), ())),
            preferred_element_type=jnp.float32,
        ).astype(qkv.dtype)
        return carry

    lax.fori_loop(0, 3, project, 0)
    for s in range(1, ns + 1):
        finish(s)
    part_rows = wo.shape[2]
    for y in range(nd):
        for e in range(nb):
            start = (y * nb + e) * part_rows
            wide_o[start : start + part_rows] = wo[y, e]

    def p_copy(c, j):
        part = pl.ds(c * CHUNK, CHUNK)
        return remote(
            p_out.at[j - 1, part], p_in.at[j - 1, part], p_send.at[c, j], p_recv.at[c, j],
            tensor=(t + j) % nt,
        )

    heads = slices // HDIM

    def partial(target):
        block = wide_o[pl.ds(pl.multiple_of(target * slices, 16), slices), :]
        return jnp.dot(block, context[...], preferred_element_type=jnp.float32).astype(own.dtype)

    def encode(c, carry):
        for i in range(CHUNK):
            here = pl.ds(pl.multiple_of((c * CHUNK + i) * patches, patches), patches)
            for h in range(heads):
                span = slice(h * HDIM, (h + 1) * HDIM)
                scores = lax.dot_general(
                    qkv[1, span, here], qkv[0, span, here], (((0,), (0,)), ((), ())),
                    preferred_element_type=jnp.float32,
                ) * HDIM ** (-0.5)
                powers = jnp.exp(scores - jnp.max(scores, axis=0, keepdims=True))
                probs = powers * (1.0 / jnp.sum(powers, axis=0, keepdims=True))
                context[span, i * patches : (i + 1) * patches] = jnp.dot(
                    qkv[2, span, here], probs.astype(qkv.dtype), preferred_element_type=jnp.float32
                ).astype(context.dtype)
        for j in range(1, nt):
            block = partial((t + j) % nt)
            for i in range(CHUNK):
                p_out[j - 1, c * CHUNK + i] = block[:, i * patches : (i + 1) * patches]
            p_copy(c, j).start()
        block = partial(t)
        for i in range(CHUNK):
            own[c * CHUNK + i] = block[:, i * patches : (i + 1) * patches]
        return carry

    lax.fori_loop(0, chunks, encode, 0)

    def close(c, carry):
        for j in range(1, nt):
            p_copy(c, j).wait_recv()
        for i in range(CHUNK):
            at = c * CHUNK + i
            total = gath[at, mine, :].astype(jnp.float32) + own[at].astype(jnp.float32)
            for j in range(1, nt):
                total = total + p_in[j - 1, at].astype(jnp.float32)
            out[at] = total.astype(out.dtype)
        return carry

    lax.fori_loop(0, chunks, close, 0)

    for c in range(chunks):
        for j in range(1, nt):
            y_copy(c, j).wait_send()
            p_copy(c, j).wait_send()
    for s, m in enumerate(bits):
        for slot in range(nb >> (s + 1)):
            for c in range(chunks):
                tile_copy(s, slot, c).wait_send()
    def drain(j, carry):
        spread(j).wait_send()
        for s in range(ns):
            for e in range(1 << s):
                doubled(j, s, e).wait_send()
        return carry

    lax.fori_loop(1, nd, drain, 0)

    def drain_line(s, carry):
        for way in range(2):
            valid, copy = line(way, s)
            pl.when(valid)(copy.wait_send)
            valid, _, half = arrival(way, s)
            if part_count > 1:
                pl.when(valid)(half.wait_send)
        return carry

    lax.fori_loop(0, nd - 1, drain_line, 0)


def encode_all(counts, ordering, tiles, qkv_weight, out_weight):
    nd, nb, nt = (lax.axis_size(name) for name in ("dp", "bal", "tensor"))
    ns = len(bits_of(nb))
    slots, slices, patches = tiles.shape
    kinds, rows, columns = qkv_weight.shape
    wq = qkv_weight.reshape(kinds, min(nb, 2), -1, columns)
    wo = out_weight.reshape(nb, -1, columns)
    chunks = CAP // CHUNK
    dtype = tiles.dtype
    vmem = pl.BlockSpec(memory_space=pltpu.VMEM)
    dma = pltpu.SemaphoreType.DMA

    def space(*shape):
        return pltpu.VMEM(shape, dtype)

    buffers = [space(nb >> (s + 1), CAP, slices, patches) for s in range(ns)]
    return pl.pallas_call(
        functools.partial(encode_kernel, (nd, nb, nt)),
        out_shape=jax.ShapeDtypeStruct((CAP, slices, patches), dtype),
        in_specs=[pl.BlockSpec(memory_space=pltpu.SMEM)] * 2 + [vmem] * 3,
        out_specs=vmem,
        scratch_shapes=buffers
        + buffers
        + [
            space(CAP, nt * slices, patches),
            space(kinds, nd, *wq.shape[1:]),
            space(nd, *wo.shape),
            space(nt * slices, columns),
            space(nt * slices, CAP * patches),
            space(kinds, columns, CAP * patches),
            space(columns, CHUNK * patches),
            space(CAP, slices, patches),
            space(max(nt - 1, 1), CAP, slices, patches),
            space(max(nt - 1, 1), CAP, slices, patches),
        ]
        + [dma((ns, max(nb // 2, 1), chunks))] * 2
        + [dma((chunks, nt))] * 2
        + [dma((nd,))] * 2
        + [dma((nd, nb))] * 2
        + [dma((chunks, nt))] * 2
        + [dma((2, nd))] * 4,
        compiler_params=pltpu.CompilerParams(
            collective_id=0, has_side_effects=True, vmem_limit_bytes=60 * 1024 * 1024
        ),
        name="encode_all",
    )(counts, ordering, tiles, wq, wo)


def local(tiles, tile_counts, doc_order, qkv_weight, out_weight):
    own_tiles = tiles[0, 0]
    return encode_all(tile_counts, doc_order, own_tiles, qkv_weight, out_weight)[None]


def solution(mesh):
    placed = (
        P("dp", "bal", None, "tensor", None),
        P("dp", None),
        P("dp", None),
        P(None, "dp", "tensor"),
        P("dp", "tensor"),
    )
    return jax.shard_map(
        local, mesh=mesh, in_specs=placed, out_specs=P("dp", "bal", "tensor", None), check_vma=False
    )
```
